128 devices in a mesh: trow: 16 (over y, x), tcol: 8 (over z, core).
Axes of the slice: x: 4, y: 4, z: 4, core: 2. Of those that a mesh axis runs over, the one named last changes fastest.
Arguments:
- left_factors: bfloat16 [2, 2, 32768, 3072], P(None, None, 'trow', 'tcol'), may hold values from -0.109375 to 0.109375
- right_factors: bfloat16 [2, 2, 12288, 8192], P(None, None, 'tcol', 'trow'), may hold values from -0.375 to 0.375
- ranks: int32 [2, 128, 48], P(None, 'trow', 'tcol'), may hold values from 4 to 64, as said below
- v_current: float32 [2, 2, 12288, 128], P(None, None, ('tcol', 'trow')), may hold values from -32 to 32
- u_prev: float32 [2, 2, 32768, 128], P(None, None, ('trow', 'tcol')), may hold values from -32 to 32
- alpha_prev: float32 [1], replicated, may hold values from 0.5 to 2
Outputs:
- u_next: float32 [2, 2, 32768, 128], P(None, None, ('trow', 'tcol'))
- v_next: float32 [2, 2, 12288, 128], P(None, None, ('tcol', 'trow'))
- scales: float32 [2], replicated
The draws below stay inside these ranges and needn't reach their ends.
Inputs may be any that keep to these rules, and one draw needn't show every extreme that they name: `ranks`: for frequency f, tile (i, j) has rank 64 // 2 + 1 to 64 where |i * 48 - j * 128| < 768, and rank 4 to 32 elsewhere.
All inputs are finite; a program needn't handle non-finite values.
Results may differ from the reference program's by a relative error of at most 0.0028.
Values may be sent and summed in bfloat16 or wider, within the bound.
No kernel may reach another device: no remote copies, remote signals or barrier semaphores. Data moves between devices by JAX's collectives and lax.ppermute only.
A program may use at most 128 MiB of HBM per device.

```python
import math
import jax
import jax.numpy as jnp
from jax import lax

F = 2
NV = 128
TILE = 256
RANK_MAX = 64
MT = 128
NT = 48
M = 32768
N = 12288


def draw_ranks(key, part):
    key_high, key_low = jax.random.split(jax.random.fold_in(key, 11))
    row_index = jnp.arange(MT, dtype=jnp.int32)[:, None]
    col_index = jnp.arange(NT, dtype=jnp.int32)[None, :]
    distance = jnp.abs(row_index * NT - col_index * MT)
    nearby = distance < MT * NT // 8
    higher = jax.random.randint(key_high, (F, MT, NT), RANK_MAX // 2 + 1, RANK_MAX + 1, dtype=jnp.int32)
    lower = jax.random.randint(key_low, (F, MT, NT), 4, RANK_MAX // 2 + 1, dtype=jnp.int32)
    return jnp.where(nearby[None], higher, lower)


def rising_field(key, rows):
    position = jnp.arange(rows, dtype=jnp.float32) / rows
    values = jax.random.normal(key, (F, 2, rows, NV), jnp.float32) * jnp.exp(jnp.log(3.0) * position)[:, None]
    values = values.at[:, :, rows - 1, 0].set(32.0)
    values = values.at[:, :, rows - 1, 1].set(-32.0)
    return jnp.clip(values, -32.0, 32.0)


def draw_v_current(key, part):
    return rising_field(jax.random.fold_in(key, 21), N)


def draw_u_prev(key, part):
    return rising_field(jax.random.fold_in(key, 31), M)


def strengthened(result, rng, source, target, parts, factor):
    owner, partner = [(jnp.arange(result.shape[dim]) // (result.shape[dim] // parts)).reshape([-1 if axis == dim else 1 for axis in range(result.ndim)]) for dim in (source, target)]
    chosen = jax.random.permutation(rng, parts)[partner]
    strong = (owner == chosen) | (owner == (partner + parts // 2) % parts)
    return jnp.where(strong, factor * result, result)


def shard_levels(own_key, dims, cuts, low, high):
    factor_of, own = 1.0, jax.random.fold_in(own_key, 6)
    for axis_at, shards_of in cuts:
        heights = jnp.exp(jax.random.uniform(jax.random.fold_in(own, axis_at), (shards_of,), jnp.float32, low / len(cuts), high / len(cuts)))
        factor_of = factor_of * jnp.repeat(heights, dims[axis_at] // shards_of).reshape([-1 if axis == axis_at else 1 for axis in range(len(dims))])
    return factor_of


def heavy_noise(rng, extent, width, bound, pieces, heavy, kind=jnp.bfloat16):
    drawn = width * jax.random.normal(rng, extent, jnp.float32)
    if pieces:
        drawn = drawn * shard_levels(rng, extent, pieces, -0.22, 0.18)
    return jnp.clip(strengthened(drawn, jax.random.fold_in(rng, 3), *heavy), -bound, bound).astype(kind)


def setup_inputs(seed: int = 0) -> dict:
    keys = jax.random.split(jax.random.key(seed), 7)
    left_factors = heavy_noise(keys[0], (F, 2, M, NT * RANK_MAX), (2 * NT * RANK_MAX) ** -0.5, 0.109375, ((2, 16), (3, 8)), (3, 2, 16, 2.0))
    right_factors = heavy_noise(keys[1], (F, 2, N, MT * RANK_MAX), (2 * TILE) ** -0.5, 0.375, ((2, 8), (3, 16)), (3, 2, 16, 2.0))
    ranks = draw_ranks(jax.random.fold_in(keys[6], 71), 0)
    v_current = draw_v_current(jax.random.fold_in(keys[6], 71), 0)
    u_prev = draw_u_prev(jax.random.fold_in(keys[6], 71), 0)
    alpha_prev = jnp.clip(jnp.exp(jax.random.uniform(keys[5], (1,), jnp.float32, math.log(0.5), math.log(2.0))), 0.5, 2.0)
    return {"left_factors": left_factors, "right_factors": right_factors, "ranks": ranks, "v_current": v_current, "u_prev": u_prev, "alpha_prev": alpha_prev}


epsilon = 1e-06

def complex_product(form, a_real, a_imag, b_real, b_imag, conjugate):
    real_real = jnp.einsum(form, a_real, b_real)
    imag_imag = jnp.einsum(form, a_imag, b_imag)
    real_imag = jnp.einsum(form, a_real, b_imag)
    imag_real = jnp.einsum(form, a_imag, b_real)
    if conjugate:
        return (real_real + imag_imag, real_imag - imag_real)
    return (real_real - imag_imag, real_imag + imag_real)

def to_float(array):
    return lax.optimization_barrier(array.astype(jnp.bfloat16)).astype(jnp.float32)

def reference(left_factors, right_factors, ranks, v_current, u_prev, alpha_prev):
    rank_mask = (jnp.arange(RANK_MAX)[None, None, None, :] < jnp.transpose(ranks, (0, 2, 1))[..., None]).astype(jnp.float32)

    def forward(items):
        left_one, right_one, mask_one, source_one = items
        right_tiles = right_one.astype(jnp.float32).reshape(2, NT, TILE, MT, RANK_MAX)
        sources = to_float(source_one).reshape(2, NT, TILE, NV)
        proj_real, proj_imag = complex_product('cmir,cmn->cirn', right_tiles[0], right_tiles[1], sources[0], sources[1], True)
        weight = mask_one[..., None]
        proj_real = to_float(proj_real * weight)
        proj_imag = to_float(proj_imag * weight)
        left_tiles = left_one.astype(jnp.float32).reshape(2, MT, TILE, NT, RANK_MAX)
        out_real, out_imag = complex_product('imcr,cirn->imn', left_tiles[0], left_tiles[1], proj_real, proj_imag, False)
        return jnp.stack([out_real, out_imag], 0).reshape(2, M, NV)
    image = lax.map(forward, (left_factors, right_factors, rank_mask, v_current))
    residual_u = image - alpha_prev[0] * u_prev
    beta_scale = jnp.sqrt(jnp.mean(residual_u * residual_u) + epsilon)
    u_next = residual_u / beta_scale

    def adjoint(items):
        left_one, right_one, mask_one, target_one = items
        left_tiles = left_one.astype(jnp.float32).reshape(2, MT, TILE, NT, RANK_MAX)
        targets = to_float(target_one).reshape(2, MT, TILE, NV)
        back_real, back_imag = complex_product('imcr,imn->cirn', left_tiles[0], left_tiles[1], targets[0], targets[1], True)
        weight = mask_one[..., None]
        back_real = to_float(back_real * weight)
        back_imag = to_float(back_imag * weight)
        right_tiles = right_one.astype(jnp.float32).reshape(2, NT, TILE, MT, RANK_MAX)
        out_real, out_imag = complex_product('cmir,cirn->cmn', right_tiles[0], right_tiles[1], back_real, back_imag, False)
        return jnp.stack([out_real, out_imag], 0).reshape(2, N, NV)
    image_back = lax.map(adjoint, (left_factors, right_factors, rank_mask, u_next))
    residual_v = image_back - beta_scale * v_current
    alpha_next = jnp.sqrt(jnp.mean(residual_v * residual_v) + epsilon)
    v_next = residual_v / alpha_next
    return (u_next, v_next, jnp.stack([beta_scale, alpha_next]))
```

```python
import functools

import jax
import jax.numpy as jnp
from jax import lax
from jax.experimental import pallas as pl
from jax.experimental.pallas import tpu as pltpu
from jax.sharding import Mesh
from jax.sharding import PartitionSpec as P

TROW = ("trow_0", "trow_1")
TCOL = ("tcol_0", "tcol_1")
TROW_TCOL = ("trow_0", "trow_1", "tcol_0", "tcol_1")
TCOL_TROW = ("tcol_0", "tcol_1", "trow_0", "trow_1")

epsilon = 1e-06
BF = jnp.bfloat16
F32 = jnp.float32
VMEM = pltpu.MemorySpace.VMEM
SMEM = pltpu.MemorySpace.SMEM
HBM = pltpu.MemorySpace.HBM


def spec(space):
    return pl.BlockSpec(memory_space=space)


def params():
    return pltpu.CompilerParams(vmem_limit_bytes=56 * 1024 * 1024)


def rank_lanes(ranks_of, count, width, rank_full):
    lane = lax.broadcasted_iota(jnp.int32, (8, width), 1)
    limit = jnp.full((8, width), ranks_of(0), jnp.int32)
    for tile in range(1, count):
        limit = jnp.where(lane >= tile * rank_full, ranks_of(tile) + tile * rank_full, limit)
    return (lane < limit)[:1]


def conjugated(stacked, real, imag, half):
    a = jnp.dot(stacked, real, preferred_element_type=F32)
    b = jnp.dot(stacked, imag, preferred_element_type=F32)
    return a[:half] + b[half:], a[half:] - b[:half]


def regroup(first, second, rank_full):
    even = jnp.concatenate([first[:, :rank_full], second[:, :rank_full]], axis=1)
    odd = jnp.concatenate([first[:, rank_full:], second[:, rank_full:]], axis=1)
    return even, odd


def turned(block, half):
    return jnp.concatenate([-block[half:], block[:half]], axis=0)


def forward_kernel(
    f, dims, where_ref, ranks_ref, source_ref, right_ref, left_ref,
    send_ref, keep_ref, right_buf, left_buf, source_t, proj, grouped, right_sem, left_sem,
):
    tile, rank_full, rows, cols, nv, share, peers = dims
    right_copies = [
        pltpu.make_async_copy(
            right_ref.at[f, :, pl.ds(j * tile, tile), :], right_buf.at[j], right_sem.at[j]
        )
        for j in range(cols)
    ]
    for copy in right_copies:
        copy.start()
    z, c = where_ref[0], where_ref[1]
    half = rows // 2
    order = [2 * lax.rem(z + d, half) + (1 - c) for d in range(half)]
    order += [2 * lax.rem(z + d, half) + c for d in range(half)]
    left_copies = [
        pltpu.make_async_copy(
            left_ref.at[f, :, pl.ds(pl.multiple_of(i * tile, tile), tile), :],
            left_buf.at[n],
            left_sem.at[n],
        )
        for n, i in enumerate(order)
    ]
    for copy in left_copies:
        copy.start()
    for r in range(peers):
        for part in range(2):
            source_t[part * nv : (part + 1) * nv, r * share : (r + 1) * share] = source_ref[r, part].T
    for j in range(cols):
        right_copies[j].wait()
        stacked = source_t[:, j * tile : (j + 1) * tile]
        real, imag = conjugated(stacked, right_buf[j, 0], right_buf[j, 1], nv)
        kept = rank_lanes(lambda i: ranks_ref[f, i, j], rows, rows * rank_full, rank_full)
        proj[j, :nv] = jnp.where(kept, real, 0.0).astype(BF)
        proj[j, nv:] = jnp.where(kept, imag, 0.0).astype(BF)
    wide = cols * rank_full
    pair = 2 * rank_full
    for j in range(0, cols, 2):
        for i in range(0, rows, 2):
            lanes = slice(i * rank_full, i * rank_full + pair)
            even, odd = regroup(proj[j, :, lanes], proj[j + 1, :, lanes], rank_full)
            at = j * rank_full
            grouped[i, :, at : at + pair] = even
            grouped[i + 1, :, at : at + pair] = odd
            grouped[i, :, wide + at : wide + at + pair] = turned(even, nv)
            grouped[i + 1, :, wide + at : wide + at + pair] = turned(odd, nv)
    for n, i in enumerate(order):
        left_copies[n].wait()
        both = jnp.concatenate([left_buf[n, 0], left_buf[n, 1]], axis=1)
        out = lax.dot_general(
            both, grouped[i], (((1,), (1,)), ((), ())), preferred_element_type=F32
        )
        if n < half:
            send_ref[n, 0] = out[:, :nv].astype(BF)
            send_ref[n, 1] = out[:, nv:].astype(BF)
        else:
            keep_ref[n - half, 0] = out[:, :nv]
            keep_ref[n - half, 1] = out[:, nv:]


def forward(f, where, ranks, source, right, left, dims):
    tile, rank_full, rows, cols, nv, share, peers = dims
    half = rows // 2
    flops = 16 * rows * cols * tile * rank_full * nv
    return pl.pallas_call(
        functools.partial(forward_kernel, f, dims),
        out_shape=(
            jax.ShapeDtypeStruct((half, 2, tile, nv), BF),
            jax.ShapeDtypeStruct((half, 2, tile, nv), F32),
        ),
        in_specs=[spec(SMEM), spec(SMEM), spec(VMEM), spec(HBM), spec(HBM)],
        out_specs=(spec(VMEM), spec(VMEM)),
        scratch_shapes=[
            pltpu.VMEM((cols, 2, tile, rows * rank_full), BF),
            pltpu.VMEM((rows, 2, tile, cols * rank_full), BF),
            pltpu.VMEM((2 * nv, cols * tile), BF),
            pltpu.VMEM((cols, 2 * nv, rows * rank_full), BF),
            pltpu.VMEM((rows, 2 * nv, 2 * cols * rank_full), BF),
            pltpu.SemaphoreType.DMA((cols,)),
            pltpu.SemaphoreType.DMA((rows,)),
        ],
        compiler_params=params(),
        cost_estimate=pl.CostEstimate(flops=flops, bytes_accessed=8_000_000, transcendentals=0),
        name=f"forward_{f}",
    )(where, ranks, source, right, left)


def adjoint_kernel(
    f, dims, where_ref, ranks_ref, right_ref, left_ref, *refs,
):
    tile, rank_full, rows, cols, nv, share, peers = dims
    targets = refs[:rows]
    out_ref, right_buf, left_buf, back, grouped, right_sem, left_sem = refs[rows:]
    z, c = where_ref[0], where_ref[1]
    half = rows // 2
    order = [2 * lax.rem(z + d, half) + c for d in range(half)]
    order += [2 * lax.rem(z + d, half) + (1 - c) for d in range(half)]
    left_copies = [
        pltpu.make_async_copy(
            left_ref.at[f, :, pl.ds(pl.multiple_of(i * tile, tile), tile), :],
            left_buf.at[n],
            left_sem.at[n],
        )
        for n, i in enumerate(order)
    ]
    for copy in left_copies:
        copy.start()
    right_copies = [
        pltpu.make_async_copy(
            right_ref.at[f, :, pl.ds(j * tile, tile), :], right_buf.at[j], right_sem.at[j]
        )
        for j in range(cols)
    ]
    for copy in right_copies:
        copy.start()
    for n, i in enumerate(order):
        left_copies[n].wait()
        real, imag = conjugated(targets[n][...], left_buf[n, 0], left_buf[n, 1], nv)
        kept = rank_lanes(lambda j: ranks_ref[f, i, j], cols, cols * rank_full, rank_full)
        back[i, :nv] = jnp.where(kept, real, 0.0).astype(BF)
        back[i, nv:] = jnp.where(kept, imag, 0.0).astype(BF)
    wide = rows * rank_full
    pair = 2 * rank_full
    for i in range(0, rows, 2):
        for j in range(0, cols, 2):
            lanes = slice(j * rank_full, j * rank_full + pair)
            even, odd = regroup(back[i, :, lanes], back[i + 1, :, lanes], rank_full)
            at = i * rank_full
            grouped[j, :, at : at + pair] = even
            grouped[j + 1, :, at : at + pair] = odd
            grouped[j, :, wide + at : wide + at + pair] = turned(even, nv)
            grouped[j + 1, :, wide + at : wide + at + pair] = turned(odd, nv)
    for j in range(cols):
        right_copies[j].wait()
        both = jnp.concatenate([right_buf[j, 0], right_buf[j, 1]], axis=1)
        out = lax.dot_general(
            both, grouped[j], (((1,), (1,)), ((), ())), preferred_element_type=F32
        ).astype(BF)
        row = 0
        while row < tile:
            whole = j * tile + row
            r, start = divmod(whole, share)
            count = min(share - start, tile - row)
            out_ref[r, 0, start : start + count] = out[row : row + count, :nv]
            out_ref[r, 1, start : start + count] = out[row : row + count, nv:]
            row += count


def adjoint(f, where, ranks, right, left, targets, dims):
    tile, rank_full, rows, cols, nv, share, peers = dims
    flops = 16 * rows * cols * tile * rank_full * nv
    return pl.pallas_call(
        functools.partial(adjoint_kernel, f, dims),
        out_shape=jax.ShapeDtypeStruct((peers, 2, share, nv), BF),
        in_specs=[spec(SMEM), spec(SMEM), spec(HBM), spec(HBM)] + [spec(VMEM)] * rows,
        out_specs=spec(VMEM),
        scratch_shapes=[
            pltpu.VMEM((cols, 2, tile, rows * rank_full), BF),
            pltpu.VMEM((rows, 2, tile, cols * rank_full), BF),
            pltpu.VMEM((rows, 2 * nv, cols * rank_full), BF),
            pltpu.VMEM((cols, 2 * nv, 2 * rows * rank_full), BF),
            pltpu.SemaphoreType.DMA((cols,)),
            pltpu.SemaphoreType.DMA((rows,)),
        ],
        compiler_params=params(),
        cost_estimate=pl.CostEstimate(flops=flops, bytes_accessed=8_000_000, transcendentals=0),
        name=f"adjoint_{f}",
    )(where, ranks, right, left, *targets)


def combine_kernel(keep_ref, other_ref, own_ref, *piece_refs):
    own_ref[...] = keep_ref[0] + other_ref[0].astype(F32)
    for d, ref in enumerate(piece_refs):
        ref[...] = (keep_ref[d + 1] + other_ref[d + 1].astype(F32)).astype(BF)


def combine(f, keep, other):
    half, _, tile, nv = keep.shape
    piece = (2, tile, nv)
    return pl.pallas_call(
        combine_kernel,
        out_shape=(jax.ShapeDtypeStruct(piece, F32),)
        + (jax.ShapeDtypeStruct(piece, BF),) * (half - 1),
        in_specs=[spec(VMEM)] * 2,
        out_specs=(spec(VMEM),) * half,
        compiler_params=params(),
        cost_estimate=pl.CostEstimate(flops=keep.size * 2, bytes_accessed=keep.size * 8, transcendentals=0),
        name=f"combine_{f}",
    )(keep, other)


def folded(value):
    return jnp.sum(value.reshape(-1, 8, value.shape[-1]), axis=0)


def residual_kernel(f, alpha_ref, u_prev_ref, own_ref, *refs):
    pieces, (res_ref, target_ref, square_ref) = refs[:-3], refs[-3:]
    total = own_ref[...] - alpha_ref[0] * u_prev_ref[f]
    for ref in pieces:
        total = total + ref[...].astype(F32)
    res_ref[...] = total
    nv = total.shape[-1]
    for part in range(2):
        target_ref[part * nv : (part + 1) * nv] = total[part].T.astype(BF)
    square_ref[...] = folded(total * total)


def residual(f, alpha_prev, u_prev, own, pieces):
    _, tile, nv = own.shape
    return pl.pallas_call(
        functools.partial(residual_kernel, f),
        out_shape=(
            jax.ShapeDtypeStruct(own.shape, F32),
            jax.ShapeDtypeStruct((2 * nv, tile), BF),
            jax.ShapeDtypeStruct((8, nv), F32),
        ),
        in_specs=[spec(SMEM)] + [spec(VMEM)] * (2 + len(pieces)),
        out_specs=(spec(VMEM),) * 3,
        compiler_params=params(),
        cost_estimate=pl.CostEstimate(flops=own.size * 8, bytes_accessed=own.size * 16, transcendentals=0),
        name=f"residual_{f}",
    )(alpha_prev, u_prev, own, *pieces)


def sums_kernel(v_ref, first_ref, second_ref, square0_ref, square1_ref, w_ref, stats_ref):
    stats = [jnp.zeros((8, v_ref.shape[-1]), F32) for _ in range(3)]
    for f, ref in enumerate((first_ref, second_ref)):
        total = ref[0].astype(F32)
        for r in range(1, ref.shape[0]):
            total = total + ref[r].astype(F32)
        w_ref[f] = total
        v = v_ref[f]
        for n, product in enumerate((total * total, total * v, v * v)):
            stats[n] = stats[n] + folded(product)
    stats.append(square0_ref[...] + square1_ref[...])
    rows = [jnp.sum(s, axis=0, keepdims=True) for s in stats]
    stats_ref[...] = jnp.concatenate(rows, axis=1)


def sums(v, first, second, square0, square1):
    nv = v.shape[-1]
    return pl.pallas_call(
        sums_kernel,
        out_shape=(jax.ShapeDtypeStruct(v.shape, F32), jax.ShapeDtypeStruct((1, 4 * nv), F32)),
        in_specs=[spec(VMEM)] * 5,
        out_specs=(spec(VMEM),) * 2,
        compiler_params=params(),
        cost_estimate=pl.CostEstimate(flops=first.size * 4, bytes_accessed=first.size * 4, transcendentals=0),
        name="sums",
    )(v, first, second, square0, square1)


def finish_kernel(count_u, count_v, all_ref, v_ref, w_ref, res0_ref, res1_ref, u_ref, next_ref, scale_ref):
    nv = v_ref.shape[-1]
    everyone = jnp.sum(all_ref[...], axis=0)
    ww, wv, vv, uu = [jnp.sum(everyone[:, n * nv : (n + 1) * nv]) for n in range(4)]
    one = jnp.ones((8, nv), F32)
    beta = jnp.sqrt(one * (uu / count_u) + epsilon)
    inverse = 1.0 / beta
    square = ww * inverse * inverse - 2.0 * wv * one + vv * beta * beta
    alpha = jnp.sqrt(jnp.maximum(square, 0.0) / count_v + epsilon)
    b, ib, ia = beta[:1], inverse[:1], (1.0 / alpha)[:1]
    for f, ref in enumerate((res0_ref, res1_ref)):
        u_ref[f] = ref[...] * ib
    next_ref[...] = (w_ref[...] * ib - v_ref[...] * b) * ia
    lane = lax.broadcasted_iota(jnp.int32, (8, nv), 1)
    scale_ref[...] = jnp.where(lane == 0, beta, alpha)


def finish(everyone, v, w, res0, res1, devices):
    nv = v.shape[-1]
    count_u = float(2 * res0.size * devices)
    count_v = float(v.size * devices)
    return pl.pallas_call(
        functools.partial(finish_kernel, count_u, count_v),
        out_shape=(
            jax.ShapeDtypeStruct((2, *res0.shape), F32),
            jax.ShapeDtypeStruct(v.shape, F32),
            jax.ShapeDtypeStruct((8, nv), F32),
        ),
        in_specs=[spec(VMEM)] * 5,
        out_specs=(spec(VMEM),) * 3,
        compiler_params=params(),
        cost_estimate=pl.CostEstimate(flops=v.size * 16, bytes_accessed=v.size * 16, transcendentals=0),
        name="finish",
    )(everyone, v, w, res0, res1)


def body(left, right, ranks, v, u_prev, alpha_prev):
    frequencies, rows, cols = ranks.shape
    tile = left.shape[2] // rows
    rank_full = left.shape[3] // cols
    nv = v.shape[3]
    peers = lax.axis_size(TROW)
    chips = lax.axis_size("tcol_0")
    devices = peers * lax.axis_size(TCOL)
    dims = (tile, rank_full, rows, cols, nv, v.shape[2], peers)
    where = jnp.stack([lax.axis_index("tcol_0"), lax.axis_index("tcol_1")]).astype(jnp.int32)
    swap = [(0, 1), (1, 0)]

    def along_z(value, step):
        return lax.ppermute(value, "tcol_0", [(i, (i + step) % chips) for i in range(chips)])

    def exchange(value, axes):
        return lax.all_to_all(value, axes, split_axis=0, concat_axis=0, tiled=True)

    source = v.astype(BF)
    results = []
    for f in range(frequencies):
        gathered = exchange(jnp.broadcast_to(source[f], (peers, *source.shape[1:])), TROW)
        send, keep = forward(f, where, ranks, gathered, right, left, dims)
        other = lax.ppermute(send, "tcol_1", swap)
        own, *pieces = combine(f, keep, other)
        arrived = [along_z(piece, d + 1) for d, piece in enumerate(pieces)]
        res, target, square = residual(f, alpha_prev, u_prev, own, arrived)
        near = [target] + [along_z(target, chips - d) for d in range(1, chips)]
        far = [lax.ppermute(value, "tcol_1", swap) for value in near]
        partial = adjoint(f, where, ranks, right, left, near + far, dims)
        results.append((res, square, exchange(partial, TROW)))
    (res0, square0, first), (res1, square1, second) = results
    w, stats = sums(v, first, second, square0, square1)
    everyone = exchange(jnp.broadcast_to(stats, (devices, *stats.shape)), TROW_TCOL)
    u_next, v_next, scales = finish(everyone, v, w, res0, res1, devices)
    return (u_next, v_next, scales[0, :2])


def solution(mesh):
    finer = Mesh(mesh.devices.reshape(4, 4, 4, 2), ("trow_0", "trow_1", "tcol_0", "tcol_1"))
    placed = (
        P(None, None, TROW, TCOL),
        P(None, None, TCOL, TROW),
        P(None, TROW, TCOL),
        P(None, None, TCOL_TROW, None),
        P(None, None, TROW_TCOL, None),
        P(),
    )
    return jax.shard_map(
        body,
        mesh=finer,
        in_specs=placed,
        out_specs=(P(None, None, TROW_TCOL, None), P(None, None, TCOL_TROW, None), P()),
        check_vma=False,
    )
```

```python
import functools

import jax
import jax.numpy as jnp
from jax import lax
from jax.experimental import pallas as pl
from jax.experimental.pallas import tpu as pltpu
from jax.sharding import Mesh
from jax.sharding import PartitionSpec as P


TROW = ("trow_0", "trow_1")
TCOL = ("tcol_0", "tcol_1")
TROW_TCOL = ("trow_0", "trow_1", "tcol_0", "tcol_1")
TCOL_TROW = ("tcol_0", "tcol_1", "trow_0", "trow_1")

epsilon = 1e-06
BF = jnp.bfloat16
F32 = jnp.float32
VMEM = pltpu.MemorySpace.VMEM
SMEM = pltpu.MemorySpace.SMEM
HBM = pltpu.MemorySpace.HBM


def spec(space):
    return pl.BlockSpec(memory_space=space)


def in_hbm(value):
    return pltpu.with_memory_space_constraint(value, HBM)


def params(mib=16):
    return pltpu.CompilerParams(vmem_limit_bytes=mib * 1024 * 1024)


def rank_lanes(ranks_of, count, width, rank_full):
    lane = lax.broadcasted_iota(jnp.int32, (8, width), 1)
    limit = jnp.full((8, width), ranks_of(0), jnp.int32)
    for tile in range(1, count):
        limit = jnp.where(lane >= tile * rank_full, ranks_of(tile) + tile * rank_full, limit)
    return (lane < limit)[:1]


def conjugated(stacked, real, imag, half):
    a = jnp.dot(stacked, real, preferred_element_type=F32)
    b = jnp.dot(stacked, imag, preferred_element_type=F32)
    return a[:half] + b[half:], a[half:] - b[:half]


def regroup(first, second, rank_full):
    even = jnp.concatenate([first[:, :rank_full], second[:, :rank_full]], axis=1)
    odd = jnp.concatenate([first[:, rank_full:], second[:, rank_full:]], axis=1)
    return even, odd


def turned(block, half):
    return jnp.concatenate([-block[half:], block[:half]], axis=0)


def run_all(copies):
    for copy in copies:
        copy.start()
    return copies


def prepare_kernel(v_ref, *refs):
    out, value, sem = refs
    value[...] = v_ref[...].astype(BF)
    peers = out.shape[0]
    for copy in run_all([pltpu.make_async_copy(value, out.at[r], sem.at[r]) for r in range(peers)]):
        copy.wait()


def prepare(v, peers):
    return pl.pallas_call(
        prepare_kernel,
        out_shape=jax.ShapeDtypeStruct((peers, *v.shape), BF),
        in_specs=[spec(VMEM)],
        out_specs=spec(HBM),
        scratch_shapes=[pltpu.VMEM(v.shape, BF), pltpu.SemaphoreType.DMA((peers,))],
        compiler_params=params(8),
        cost_estimate=pl.CostEstimate(flops=v.size, bytes_accessed=v.size * 36, transcendentals=0),
        name="prepare",
    )(v)


def tile_rows(index, tile):
    return pl.ds(pl.multiple_of(index * tile, tile), tile)


def tile_copies(factor_ref, f, indices, tile, out, sem):
    return [
        pltpu.make_async_copy(factor_ref.at[f, :, tile_rows(index, tile), :], out.at[n], sem.at[n])
        for n, index in enumerate(indices)
    ]


def order_of(where_ref, half):
    z, c = where_ref[0], where_ref[1]
    chips = [2 * lax.rem(z + d, half) for d in range(half)]
    return [chip + c for chip in chips], [chip + (1 - c) for chip in chips]


def expanded(factor, grouped):
    both = jnp.concatenate([factor[0], factor[1]], axis=1)
    return lax.dot_general(both, grouped, (((1,), (1,)), ((), ())), preferred_element_type=F32)


def project_kernel(
    f, dims, where_ref, ranks_ref, source_ref, right_ref, left_ref,
    send_ref, kept_ref, kept_left_ref,
    right_buf, left_buf, source_t, proj, grouped, right_sem, left_sem, kept_sem,
):
    tile, rank_full, rows, cols, nv, share, peers = dims
    half = rows // 2
    near, far = order_of(where_ref, half)
    rights = run_all(tile_copies(right_ref, f, range(cols), tile, right_buf, right_sem))
    lefts = run_all(tile_copies(left_ref, f, far, tile, left_buf, left_sem))
    kept_lefts = run_all(tile_copies(left_ref, f, near, tile, kept_left_ref, kept_sem))
    for r in range(peers):
        for part in range(2):
            source_t[part * nv : (part + 1) * nv, r * share : (r + 1) * share] = source_ref[r, f, part].T
    for j in range(cols):
        rights[j].wait()
        stacked = source_t[:, j * tile : (j + 1) * tile]
        real, imag = conjugated(stacked, right_buf[j, 0], right_buf[j, 1], nv)
        kept = rank_lanes(lambda i: ranks_ref[f, i, j], rows, rows * rank_full, rank_full)
        proj[j, :nv] = jnp.where(kept, real, 0.0).astype(BF)
        proj[j, nv:] = jnp.where(kept, imag, 0.0).astype(BF)
    wide = cols * rank_full
    pair = 2 * rank_full
    for j in range(0, cols, 2):
        for i in range(0, rows, 2):
            lanes = slice(i * rank_full, i * rank_full + pair)
            even, odd = regroup(proj[j, :, lanes], proj[j + 1, :, lanes], rank_full)
            at = j * rank_full
            grouped[i, :, at : at + pair] = even
            grouped[i + 1, :, at : at + pair] = odd
            grouped[i, :, wide + at : wide + at + pair] = turned(even, nv)
            grouped[i + 1, :, wide + at : wide + at + pair] = turned(odd, nv)
    for d in range(half):
        lefts[d].wait()
        out = expanded(left_buf[d], grouped[far[d]])
        send_ref[d, 0] = out[:, :nv].astype(BF)
        send_ref[d, 1] = out[:, nv:].astype(BF)
        kept_ref[d] = grouped[near[d]]
    for copy in kept_lefts:
        copy.wait()


def project(f, where, ranks, source, right, left, dims):
    tile, rank_full, rows, cols, nv, _, _ = dims
    half = rows // 2
    flops = 12 * rows * cols * tile * rank_full * nv
    left_tiles = (half, 2, tile, cols * rank_full)
    return pl.pallas_call(
        functools.partial(project_kernel, f, dims),
        out_shape=(
            jax.ShapeDtypeStruct((half, 2, tile, nv), BF),
            jax.ShapeDtypeStruct((half, 2 * nv, 2 * cols * rank_full), BF),
            jax.ShapeDtypeStruct(left_tiles, BF),
        ),
        in_specs=[spec(SMEM), spec(SMEM), spec(VMEM), spec(HBM), spec(HBM)],
        out_specs=(spec(VMEM),) * 3,
        scratch_shapes=[
            pltpu.VMEM((cols, 2, tile, rows * rank_full), BF),
            pltpu.VMEM(left_tiles, BF),
            pltpu.VMEM((2 * nv, cols * tile), BF),
            pltpu.VMEM((cols, 2 * nv, rows * rank_full), BF),
            pltpu.VMEM((rows, 2 * nv, 2 * cols * rank_full), BF),
            pltpu.SemaphoreType.DMA((cols,)),
            pltpu.SemaphoreType.DMA((half,)),
            pltpu.SemaphoreType.DMA((half,)),
        ],
        compiler_params=params(24),
        cost_estimate=pl.CostEstimate(flops=flops, bytes_accessed=8_000_000, transcendentals=0),
    )(where, ranks, source, in_hbm(right), in_hbm(left))


def expand_kernel(dims, kept_ref, other_ref, left_ref, own_ref, *piece_refs):
    nv, half = dims[4], dims[2] // 2
    for d in list(range(1, half)) + [0]:
        out = expanded(left_ref[d], kept_ref[d])
        for part in range(2):
            total = out[:, part * nv : (part + 1) * nv] + other_ref[d, part].astype(F32)
            if d == 0:
                own_ref[part] = total
            else:
                piece_refs[d - 1][part] = total.astype(BF)


def expand(kept, other, left, dims):
    tile, rank_full, rows, cols, nv, _, _ = dims
    half = rows // 2
    piece = (2, tile, nv)
    return pl.pallas_call(
        functools.partial(expand_kernel, dims),
        out_shape=(jax.ShapeDtypeStruct(piece, F32),)
        + (jax.ShapeDtypeStruct(piece, BF),) * (half - 1),
        in_specs=[spec(VMEM)] * 3,
        out_specs=(spec(VMEM),) * half,
        compiler_params=params(),
        cost_estimate=pl.CostEstimate(
            flops=4 * rows * cols * tile * rank_full * nv, bytes_accessed=4_000_000, transcendentals=0
        ),
    )(kept, other, left)


def back_of(f, index, target, left, ranks_ref, dims):
    _, rank_full, _, cols, nv, _, _ = dims
    real, imag = conjugated(target, left[0], left[1], nv)
    kept = rank_lanes(lambda j: ranks_ref[f, index, j], cols, cols * rank_full, rank_full)
    return jnp.where(kept, real, 0.0).astype(BF), jnp.where(kept, imag, 0.0).astype(BF)


def near_kernel(f, dims, where_ref, ranks_ref, right_ref, left_ref, *refs):
    tile, _, rows, cols, nv, _, _ = dims
    half = rows // 2
    targets = refs[:half]
    back_ref, right_out, left_out, left_buf, left_sem, far_sem, right_sem = refs[half:]
    near, far = order_of(where_ref, half)
    lefts = run_all(tile_copies(left_ref, f, near, tile, left_buf, left_sem))
    later = run_all(tile_copies(left_ref, f, far, tile, left_out, far_sem))
    later += run_all(tile_copies(right_ref, f, range(cols), tile, right_out, right_sem))
    for d, target in enumerate(targets):
        lefts[d].wait()
        real, imag = back_of(f, near[d], target[...], left_buf[d], ranks_ref, dims)
        back_ref[d, :nv] = real
        back_ref[d, nv:] = imag
    for copy in later:
        copy.wait()


def near_back(f, where, ranks, right, left, targets, dims):
    tile, rank_full, rows, cols, nv, _, _ = dims
    half = rows // 2
    left_tiles = (half, 2, tile, cols * rank_full)
    return pl.pallas_call(
        functools.partial(near_kernel, f, dims),
        out_shape=(
            jax.ShapeDtypeStruct((half, 2 * nv, cols * rank_full), BF),
            jax.ShapeDtypeStruct((cols, 2, tile, rows * rank_full), BF),
            jax.ShapeDtypeStruct(left_tiles, BF),
        ),
        in_specs=[spec(SMEM), spec(SMEM), spec(HBM), spec(HBM)] + [spec(VMEM)] * half,
        out_specs=(spec(VMEM),) * 3,
        scratch_shapes=[
            pltpu.VMEM(left_tiles, BF),
            pltpu.SemaphoreType.DMA((half,)),
            pltpu.SemaphoreType.DMA((half,)),
            pltpu.SemaphoreType.DMA((cols,)),
        ],
        compiler_params=params(24),
        cost_estimate=pl.CostEstimate(
            flops=4 * rows * cols * tile * rank_full * nv, bytes_accessed=4_000_000, transcendentals=0
        ),
    )(where, ranks, in_hbm(right), in_hbm(left), *targets)


def adjoint_kernel(f, dims, where_ref, ranks_ref, near_ref, right_ref, left_ref, *refs):
    tile, rank_full, rows, cols, nv, share, _ = dims
    half = rows // 2
    targets = refs[:half]
    out_hbm, back, grouped, out_ref, out_sem = refs[half:]
    near, far = order_of(where_ref, half)
    for d in range(half):
        back[near[d]] = near_ref[d]
        real, imag = back_of(f, far[d], targets[d][...], left_ref[d], ranks_ref, dims)
        back[far[d], :nv] = real
        back[far[d], nv:] = imag
    wide = rows * rank_full
    pair = 2 * rank_full
    for i in range(0, rows, 2):
        for j in range(0, cols, 2):
            lanes = slice(j * rank_full, j * rank_full + pair)
            even, odd = regroup(back[i, :, lanes], back[i + 1, :, lanes], rank_full)
            at = i * rank_full
            grouped[j, :, at : at + pair] = even
            grouped[j + 1, :, at : at + pair] = odd
            grouped[j, :, wide + at : wide + at + pair] = turned(even, nv)
            grouped[j + 1, :, wide + at : wide + at + pair] = turned(odd, nv)
    copies = []
    for j in range(cols):
        out = expanded(right_ref[j], grouped[j]).astype(BF)
        row = 0
        while row < tile:
            r, start = divmod(j * tile + row, share)
            count = min(share - start, tile - row)
            out_ref[r, 0, start : start + count] = out[row : row + count, :nv]
            out_ref[r, 1, start : start + count] = out[row : row + count, nv:]
            row += count
            if start + count == share:
                copies += run_all([pltpu.make_async_copy(out_ref.at[r], out_hbm.at[r], out_sem.at[r])])
    for copy in copies:
        copy.wait()


def adjoint(f, where, ranks, near, right, left, targets, dims):
    tile, rank_full, rows, cols, nv, share, peers = dims
    flops = 12 * rows * cols * tile * rank_full * nv
    return pl.pallas_call(
        functools.partial(adjoint_kernel, f, dims),
        out_shape=jax.ShapeDtypeStruct((peers, 2, share, nv), BF),
        in_specs=[spec(SMEM), spec(SMEM)] + [spec(VMEM)] * (3 + len(targets)),
        out_specs=spec(HBM),
        scratch_shapes=[
            pltpu.VMEM((rows, 2 * nv, cols * rank_full), BF),
            pltpu.VMEM((cols, 2 * nv, 2 * rows * rank_full), BF),
            pltpu.VMEM((peers, 2, share, nv), BF),
            pltpu.SemaphoreType.DMA((peers,)),
        ],
        compiler_params=params(),
        cost_estimate=pl.CostEstimate(flops=flops, bytes_accessed=8_000_000, transcendentals=0),
    )(where, ranks, near, right, left, *targets)


def folded(value):
    return jnp.sum(value.reshape(-1, 8, value.shape[-1]), axis=0)


def residual_kernel(f, alpha_ref, u_prev_ref, own_ref, *refs):
    pieces, (res_ref, target_ref, square_ref) = refs[:-3], refs[-3:]
    total = own_ref[...] - alpha_ref[0] * u_prev_ref[f]
    for ref in pieces:
        total = total + ref[...].astype(F32)
    res_ref[...] = total
    nv = total.shape[-1]
    for part in range(2):
        target_ref[part * nv : (part + 1) * nv] = total[part].T.astype(BF)
    square_ref[...] = folded(total * total)


def residual(f, alpha_prev, u_prev, own, pieces):
    _, tile, nv = own.shape
    return pl.pallas_call(
        functools.partial(residual_kernel, f),
        out_shape=(
            jax.ShapeDtypeStruct(own.shape, F32),
            jax.ShapeDtypeStruct((2 * nv, tile), BF),
            jax.ShapeDtypeStruct((8, nv), F32),
        ),
        in_specs=[spec(SMEM)] + [spec(VMEM)] * (2 + len(pieces)),
        out_specs=(spec(VMEM),) * 3,
        compiler_params=params(),
        cost_estimate=pl.CostEstimate(flops=own.size * 8, bytes_accessed=own.size * 16, transcendentals=0),
    )(alpha_prev, u_prev, own, *pieces)


def lane_sums(stats):
    nv = stats[0].shape[-1]
    lane = lax.broadcasted_iota(jnp.int32, (1, nv), 1)
    row = jnp.zeros((1, nv), F32)
    for n, value in enumerate(stats):
        total = jnp.sum(jnp.sum(value, axis=0, keepdims=True), axis=1, keepdims=True)
        row = jnp.where(lane == n, total, row)
    return row


def sums_kernel(f, v_ref, partial_ref, square_ref, *refs):
    w_ref, stats_ref = refs[-2:]
    total = partial_ref[0].astype(F32)
    for r in range(1, partial_ref.shape[0]):
        total = total + partial_ref[r].astype(F32)
    w_ref[...] = total
    v = v_ref[f]
    row = lane_sums([folded(total * total), folded(total * v), folded(v * v), square_ref[...]])
    stats_ref[...] = row + refs[0][...] if len(refs) == 3 else row


def sums(f, v, partial, square, before):
    nv = v.shape[-1]
    return pl.pallas_call(
        functools.partial(sums_kernel, f),
        out_shape=(jax.ShapeDtypeStruct(v.shape[1:], F32), jax.ShapeDtypeStruct((1, nv), F32)),
        in_specs=[spec(VMEM)] * (3 + len(before)),
        out_specs=(spec(VMEM),) * 2,
        compiler_params=params(),
        cost_estimate=pl.CostEstimate(flops=partial.size * 2, bytes_accessed=partial.size * 2, transcendentals=0),
    )(v, partial, square, *before)


def finish_kernel(count_u, count_v, all_ref, v_ref, w0_ref, w1_ref, res0_ref, res1_ref, u_ref, next_ref, scale_ref):
    nv = v_ref.shape[-1]
    everyone = jnp.sum(all_ref[...], axis=0)
    ww, wv, vv, uu = [everyone[:, n : n + 1] for n in range(4)]
    beta = jnp.sqrt(uu / count_u + epsilon)
    inverse = 1.0 / beta
    square = ww * inverse * inverse - 2.0 * wv + vv * beta * beta
    alpha = jnp.sqrt(jnp.maximum(square, 0.0) / count_v + epsilon)
    spread = [jnp.broadcast_to(x, (1, nv)) for x in (beta, inverse, 1.0 / alpha)]
    b, ib, ia = spread
    for f, (res_ref, w_ref) in enumerate(((res0_ref, w0_ref), (res1_ref, w1_ref))):
        u_ref[f] = res_ref[...] * ib
        next_ref[f] = (w_ref[...] * ib - v_ref[f] * b) * ia
    scale_ref[0] = beta[0, 0]
    scale_ref[1] = alpha[0, 0]


def finish(everyone, v, w0, w1, res0, res1, devices):
    count_u = float(2 * res0.size * devices)
    count_v = float(v.size * devices)
    return pl.pallas_call(
        functools.partial(finish_kernel, count_u, count_v),
        out_shape=(
            jax.ShapeDtypeStruct((2, *res0.shape), F32),
            jax.ShapeDtypeStruct(v.shape, F32),
            jax.ShapeDtypeStruct((2,), F32),
        ),
        in_specs=[spec(VMEM)] * 6,
        out_specs=(spec(VMEM), spec(VMEM), spec(SMEM)),
        compiler_params=params(),
        cost_estimate=pl.CostEstimate(flops=v.size * 16, bytes_accessed=v.size * 16, transcendentals=0),
        name="finish",
    )(everyone, v, w0, w1, res0, res1)


def body(left, right, ranks, v, u_prev, alpha_prev):
    frequencies, rows, cols = ranks.shape
    tile = left.shape[2] // rows
    rank_full = left.shape[3] // cols
    nv = v.shape[3]
    peers = lax.axis_size(TROW)
    chips = lax.axis_size("tcol_0")
    devices = peers * lax.axis_size(TCOL)
    dims = (tile, rank_full, rows, cols, nv, v.shape[2], peers)
    where = jnp.stack([lax.axis_index("tcol_0"), lax.axis_index("tcol_1")]).astype(jnp.int32)
    swap = [(0, 1), (1, 0)]

    def along_z(value, step):
        return lax.ppermute(value, "tcol_0", [(i, (i + step) % chips) for i in range(chips)])

    def exchange(value, axes):
        return lax.all_to_all(value, axes, split_axis=0, concat_axis=0, tiled=True)

    source = prepare(v, peers)
    gathered = exchange(source, TROW)
    results = []
    for f in range(frequencies):
        send, kept, kept_left = project(f, where, ranks, gathered, right, left, dims)
        other = lax.ppermute(send, "tcol_1", swap)
        own, *pieces = expand(kept, other, kept_left, dims)
        arrived = []
        for d, piece in enumerate(pieces):
            arrived.append(along_z(piece, d + 1))
        res, target, square = residual(f, alpha_prev, u_prev, own, arrived)
        near = [target]
        for d in range(1, chips):
            near.append(along_z(target, chips - d))
        far = []
        for d in range(chips):
            far.append(lax.ppermute(near[d], "tcol_1", swap))
        back, far_right, far_left = near_back(f, where, ranks, right, left, near, dims)
        partial = adjoint(f, where, ranks, back, far_right, far_left, far, dims)
        results.append((res, square, exchange(partial, TROW)))
    (res0, square0, first), (res1, square1, second) = results
    w0, stats0 = sums(0, v, first, square0, ())
    w1, stats = sums(1, v, second, square1, (stats0,))
    everyone = exchange(jnp.broadcast_to(stats, (devices, *stats.shape)), TROW_TCOL)
    return finish(everyone, v, w0, w1, res0, res1, devices)


def solution(mesh):
    finer = Mesh(mesh.devices.reshape(4, 4, 4, 2), ("trow_0", "trow_1", "tcol_0", "tcol_1"))
    placed = (
        P(None, None, TROW, TCOL),
        P(None, None, TCOL, TROW),
        P(None, TROW, TCOL),
        P(None, None, TCOL_TROW, None),
        P(None, None, TROW_TCOL, None),
        P(),
    )
    return jax.shard_map(
        body,
        mesh=finer,
        in_specs=placed,
        out_specs=(P(None, None, TROW_TCOL, None), P(None, None, TCOL_TROW, None), P()),
        check_vma=False,
    )
```

```python
import functools

import jax
import jax.numpy as jnp
from jax import lax
from jax.experimental import pallas as pl
from jax.experimental.pallas import tpu as pltpu
from jax.sharding import Mesh
from jax.sharding import PartitionSpec as P


TROW = ("trow_0", "trow_1")
TCOL = ("tcol_0", "tcol_1")
TROW_TCOL = ("trow_0", "trow_1", "tcol_0", "tcol_1")
TCOL_TROW = ("tcol_0", "tcol_1", "trow_0", "trow_1")

epsilon = 1e-06
BF = jnp.bfloat16
F32 = jnp.float32
VMEM = pltpu.MemorySpace.VMEM
SMEM = pltpu.MemorySpace.SMEM
HBM = pltpu.MemorySpace.HBM


def spec(space):
    return pl.BlockSpec(memory_space=space)


def in_hbm(value):
    return pltpu.with_memory_space_constraint(value, HBM)


def params(mib=16):
    return pltpu.CompilerParams(vmem_limit_bytes=mib * 1024 * 1024)


def rank_lanes(ranks_of, count, width, rank_full):
    lane = lax.broadcasted_iota(jnp.int32, (8, width), 1)
    limit = jnp.full((8, width), ranks_of(0), jnp.int32)
    for tile in range(1, count):
        limit = jnp.where(lane >= tile * rank_full, ranks_of(tile) + tile * rank_full, limit)
    return (lane < limit)[:1]


def conjugated(stacked, real, imag, half):
    a = jnp.dot(stacked, real, preferred_element_type=F32)
    b = jnp.dot(stacked, imag, preferred_element_type=F32)
    return a[:half] + b[half:], a[half:] - b[:half]


def regroup(first, second, rank_full):
    even = jnp.concatenate([first[:, :rank_full], second[:, :rank_full]], axis=1)
    odd = jnp.concatenate([first[:, rank_full:], second[:, rank_full:]], axis=1)
    return even, odd


def turned(block, half):
    return jnp.concatenate([-block[half:], block[:half]], axis=0)


def prepare_kernel(v_ref, *out_refs):
    for f, ref in enumerate(out_refs):
        value = v_ref[f].astype(BF)
        for r in range(ref.shape[0]):
            ref[r] = value


def prepare(v, peers):
    frequencies = v.shape[0]
    return pl.pallas_call(
        prepare_kernel,
        out_shape=(jax.ShapeDtypeStruct((peers, *v.shape[1:]), BF),) * frequencies,
        in_specs=[spec(VMEM)],
        out_specs=(spec(VMEM),) * frequencies,
        compiler_params=params(8),
        cost_estimate=pl.CostEstimate(flops=v.size, bytes_accessed=v.size * 36, transcendentals=0),
        name="prepare",
    )(v)


def run_all(copies):
    for copy in copies:
        copy.start()
    return copies


def wait_all(copies):
    for copy in copies:
        copy.wait()


def tile_copies(factor_ref, f, indices, tile, out, sem):
    copies = []
    for n, index in enumerate(indices):
        at = pl.ds(pl.multiple_of(index * tile, tile), tile)
        copies.append(pltpu.make_async_copy(factor_ref.at[f, :, at, :], out.at[n], sem.at[n]))
    return copies


def sides(core_ref, half):
    z, c = core_ref[0], core_ref[1]
    chips = [2 * lax.rem(z + d, half) for d in range(half)]
    return [chip + c for chip in chips], [chip + (1 - c) for chip in chips]


def expanded(factor, grouped):
    both = jnp.concatenate([factor[0], factor[1]], axis=1)
    return lax.dot_general(both, grouped, (((1,), (1,)), ((), ())), preferred_element_type=F32)


def masked(kept, real, imag):
    return jnp.where(kept, real, 0.0).astype(BF), jnp.where(kept, imag, 0.0).astype(BF)


def regroup_all(blocks, grouped, outer, inner, rank_full, nv):
    wide = outer * rank_full
    pair = 2 * rank_full
    for o in range(0, outer, 2):
        for i in range(0, inner, 2):
            lanes = slice(i * rank_full, i * rank_full + pair)
            even, odd = regroup(blocks[o, :, lanes], blocks[o + 1, :, lanes], rank_full)
            at = o * rank_full
            for n, block in enumerate((even, odd)):
                grouped[i + n, :, at : at + pair] = block
                grouped[i + n, :, wide + at : wide + at + pair] = turned(block, nv)


def projected(f, dims, near, far, ranks_ref, source_ref, right, ready, left, left_ready, out_refs, scratch):
    tile, rank_full, rows, cols, nv, share, peers = dims
    send_ref, kept_ref = out_refs
    stored, proj, grouped = scratch
    for r in range(peers):
        for part in range(2):
            stored[part, r * share : (r + 1) * share, :] = source_ref[r, part]
    for j in range(cols):
        at = slice(j * tile, (j + 1) * tile)
        stacked = jnp.concatenate([stored[0, at].T, stored[1, at].T], axis=0)
        ready(j)
        real, imag = conjugated(stacked, right[j, 0], right[j, 1], nv)
        kept = rank_lanes(lambda i: ranks_ref[f, i, j], rows, rows * rank_full, rank_full)
        proj[j, :nv], proj[j, nv:] = masked(kept, real, imag)
    regroup_all(proj, grouped, cols, rows, rank_full, nv)
    for d in range(rows // 2):
        left_ready(d)
        out = expanded(left[d], grouped[far[d]])
        send_ref[d, 0] = out[:, :nv].astype(BF)
        send_ref[d, 1] = out[:, nv:].astype(BF)
        kept_ref[d] = grouped[near[d]]


def project_kernel(
    f, dims, core_ref, ranks_ref, source_ref, right_ref, left_ref,
    send_ref, kept_ref, near_left_ref,
    right_buf, left_buf, stored, proj, grouped, right_sem, left_sem, near_sem,
):
    tile, rows, cols = dims[0], dims[2], dims[3]
    near, far = sides(core_ref, rows // 2)
    rights = run_all(tile_copies(right_ref, f, range(cols), tile, right_buf, right_sem))
    lefts = tile_copies(left_ref, f, far, tile, left_buf, left_sem)
    later = tile_copies(left_ref, f, near, tile, near_left_ref, near_sem)

    def ready(j):
        rights[j].wait()
        if j == 0:
            run_all(lefts)
            run_all(later)

    projected(
        f, dims, near, far, ranks_ref, source_ref, right_buf, ready, left_buf,
        lambda d: lefts[d].wait(), (send_ref, kept_ref), (stored, proj, grouped),
    )
    wait_all(later)


def project_shapes(dims):
    tile, rank_full, rows, cols, nv, _, _ = dims
    half = rows // 2
    shapes = {
        "send": (half, 2, tile, nv),
        "kept": (half, 2 * nv, 2 * cols * rank_full),
        "left": (half, 2, tile, cols * rank_full),
        "right": (cols, 2, tile, rows * rank_full),
    }
    scratch = [
        pltpu.VMEM((2, cols * tile, nv), BF),
        pltpu.VMEM((cols, 2 * nv, rows * rank_full), BF),
        pltpu.VMEM((rows, 2 * nv, 2 * cols * rank_full), BF),
    ]
    return shapes, scratch, pl.CostEstimate(
        flops=12 * rows * cols * tile * rank_full * nv, bytes_accessed=8_000_000, transcendentals=0
    )


def project(f, core, ranks, source, right, left, dims):
    shapes, scratch, cost = project_shapes(dims)
    half, cols = dims[2] // 2, dims[3]
    outs = ("send", "kept", "left")
    sem = pltpu.SemaphoreType.DMA
    return pl.pallas_call(
        functools.partial(project_kernel, f, dims),
        out_shape=tuple(jax.ShapeDtypeStruct(shapes[n], BF) for n in outs),
        in_specs=[spec(SMEM), spec(SMEM), spec(VMEM), spec(HBM), spec(HBM)],
        out_specs=(spec(VMEM),) * len(outs),
        scratch_shapes=[pltpu.VMEM(shapes["right"], BF), pltpu.VMEM(shapes["left"], BF)]
        + scratch
        + [sem((cols,)), sem((half,)), sem((half,))],
        compiler_params=params(20),
        cost_estimate=cost,
    )(core, ranks, source, in_hbm(right), in_hbm(left))


def expand_kernel(dims, kept_ref, other_ref, left_ref, own_ref, *piece_refs):
    nv, half = dims[4], dims[2] // 2
    for d in list(range(1, half)) + [0]:
        out = expanded(left_ref[d], kept_ref[d])
        for part in range(2):
            total = out[:, part * nv : (part + 1) * nv] + other_ref[d, part].astype(F32)
            if d == 0:
                own_ref[part] = total
            else:
                piece_refs[d - 1][part] = total.astype(BF)


def expand(kept, other, left, dims):
    tile, rank_full, rows, cols, nv, _, _ = dims
    half = rows // 2
    piece = (2, tile, nv)
    return pl.pallas_call(
        functools.partial(expand_kernel, dims),
        out_shape=(jax.ShapeDtypeStruct(piece, F32),)
        + (jax.ShapeDtypeStruct(piece, BF),) * (half - 1),
        in_specs=[spec(VMEM)] * 3,
        out_specs=(spec(VMEM),) * half,
        compiler_params=params(),
        cost_estimate=pl.CostEstimate(
            flops=4 * rows * cols * tile * rank_full * nv, bytes_accessed=4_000_000, transcendentals=0
        ),
    )(kept, other, left)


def back_of(f, index, target, left, ranks_ref, dims):
    _, rank_full, _, cols, nv, _, _ = dims
    real, imag = conjugated(target, left[0], left[1], nv)
    kept = rank_lanes(lambda j: ranks_ref[f, index, j], cols, cols * rank_full, rank_full)
    return masked(kept, real, imag)


def near_kernel(
    f, dims, core_ref, ranks_ref, right_ref, left_ref, *refs,
):
    tile, _, rows, cols, nv, _, _ = dims
    half = rows // 2
    targets = refs[:half]
    back_ref, right_out, far_out, left_buf, left_sem, far_sem, right_sem = refs[half:]
    near, far = sides(core_ref, half)
    lefts = run_all(tile_copies(left_ref, f, near, tile, left_buf, left_sem))
    later = run_all(tile_copies(left_ref, f, far, tile, far_out, far_sem))
    later += run_all(tile_copies(right_ref, f, range(cols), tile, right_out, right_sem))
    for d in range(half):
        lefts[d].wait()
        real, imag = back_of(f, near[d], targets[d][...], left_buf[d], ranks_ref, dims)
        back_ref[d, :nv] = real
        back_ref[d, nv:] = imag
    wait_all(later)


def near_back(f, core, ranks, targets, right, left, dims):
    tile, rank_full, rows, cols, nv, _, _ = dims
    half = rows // 2
    left_tiles = (half, 2, tile, cols * rank_full)
    return pl.pallas_call(
        functools.partial(near_kernel, f, dims),
        out_shape=(
            jax.ShapeDtypeStruct((half, 2 * nv, cols * rank_full), BF),
            jax.ShapeDtypeStruct((cols, 2, tile, rows * rank_full), BF),
            jax.ShapeDtypeStruct(left_tiles, BF),
        ),
        in_specs=[spec(SMEM), spec(SMEM), spec(HBM), spec(HBM)] + [spec(VMEM)] * half,
        out_specs=(spec(VMEM),) * 3,
        scratch_shapes=[
            pltpu.VMEM(left_tiles, BF),
            pltpu.SemaphoreType.DMA((half,)),
            pltpu.SemaphoreType.DMA((half,)),
            pltpu.SemaphoreType.DMA((cols,)),
        ],
        compiler_params=params(16),
        cost_estimate=pl.CostEstimate(
            flops=4 * rows * cols * tile * rank_full * nv, bytes_accessed=8_000_000, transcendentals=0
        ),
    )(core, ranks, in_hbm(right), in_hbm(left), *targets)


def adjoint_kernel(f, dims, core_ref, ranks_ref, near_ref, right_ref, far_left_ref, *refs):
    tile, rank_full, rows, cols, nv, share, _ = dims
    half = rows // 2
    targets = refs[:half]
    out_hbm, back, grouped, out_ref, out_sem = refs[half:]
    near, far = sides(core_ref, half)
    for d in range(half):
        back[near[d]] = near_ref[d]
        real, imag = back_of(f, far[d], targets[d][...], far_left_ref[d], ranks_ref, dims)
        back[far[d], :nv] = real
        back[far[d], nv:] = imag
    regroup_all(back, grouped, rows, cols, rank_full, nv)
    copies = []
    for j in range(cols):
        out = expanded(right_ref[j], grouped[j]).astype(BF)
        row = 0
        while row < tile:
            r, start = divmod(j * tile + row, share)
            count = min(share - start, tile - row)
            for part in range(2):
                out_ref[r, part, start : start + count] = out[row : row + count, part * nv : (part + 1) * nv]
            row += count
            if start + count == share:
                copies += run_all([pltpu.make_async_copy(out_ref.at[r], out_hbm.at[r], out_sem.at[r])])
    wait_all(copies)


def adjoint(f, core, ranks, near, right, far_left, targets, dims):
    tile, rank_full, rows, cols, nv, share, peers = dims
    return pl.pallas_call(
        functools.partial(adjoint_kernel, f, dims),
        out_shape=jax.ShapeDtypeStruct((peers, 2, share, nv), BF),
        in_specs=[spec(SMEM), spec(SMEM)] + [spec(VMEM)] * (3 + len(targets)),
        out_specs=spec(HBM),
        scratch_shapes=[
            pltpu.VMEM((rows, 2 * nv, cols * rank_full), BF),
            pltpu.VMEM((cols, 2 * nv, 2 * rows * rank_full), BF),
            pltpu.VMEM((peers, 2, share, nv), BF),
            pltpu.SemaphoreType.DMA((peers,)),
        ],
        compiler_params=params(16),
        cost_estimate=pl.CostEstimate(
            flops=12 * rows * cols * tile * rank_full * nv, bytes_accessed=8_000_000, transcendentals=0
        ),
    )(core, ranks, near, right, far_left, *targets)


def folded(value):
    return jnp.sum(value.reshape(-1, 8, value.shape[-1]), axis=0)


def residual_kernel(f, alpha_ref, u_prev_ref, own_ref, *refs):
    pieces, (res_ref, target_ref, square_ref) = refs[:-3], refs[-3:]
    total = own_ref[...] - alpha_ref[0] * u_prev_ref[f]
    for ref in pieces:
        total = total + ref[...].astype(F32)
    res_ref[...] = total
    nv = total.shape[-1]
    for part in range(2):
        target_ref[part * nv : (part + 1) * nv] = total[part].T.astype(BF)
    square_ref[...] = folded(total * total)


def residual(f, alpha_prev, u_prev, own, pieces):
    _, tile, nv = own.shape
    return pl.pallas_call(
        functools.partial(residual_kernel, f),
        out_shape=(
            jax.ShapeDtypeStruct(own.shape, F32),
            jax.ShapeDtypeStruct((2 * nv, tile), BF),
            jax.ShapeDtypeStruct((8, nv), F32),
        ),
        in_specs=[spec(SMEM)] + [spec(VMEM)] * (2 + len(pieces)),
        out_specs=(spec(VMEM),) * 3,
        compiler_params=params(),
        cost_estimate=pl.CostEstimate(flops=own.size * 8, bytes_accessed=own.size * 16, transcendentals=0),
    )(alpha_prev, u_prev, own, *pieces)


def lane_sums(stats):
    nv = stats[0].shape[-1]
    lane = lax.broadcasted_iota(jnp.int32, (1, nv), 1)
    row = jnp.zeros((1, nv), F32)
    for n, value in enumerate(stats):
        total = jnp.sum(jnp.sum(value, axis=0, keepdims=True), axis=1, keepdims=True)
        row = jnp.where(lane == n, total, row)
    return row


def sums_kernel(f, v_ref, partial_ref, square_ref, *refs):
    w_ref, stats_ref = refs[-2:]
    total = partial_ref[0].astype(F32)
    for r in range(1, partial_ref.shape[0]):
        total = total + partial_ref[r].astype(F32)
    w_ref[...] = total
    v = v_ref[f]
    row = lane_sums([folded(total * total), folded(total * v), folded(v * v), square_ref[...]])
    stats_ref[...] = row + refs[0][...] if len(refs) == 3 else row


def sums(f, v, partial, square, before):
    nv = v.shape[-1]
    return pl.pallas_call(
        functools.partial(sums_kernel, f),
        out_shape=(jax.ShapeDtypeStruct(v.shape[1:], F32), jax.ShapeDtypeStruct((1, nv), F32)),
        in_specs=[spec(VMEM)] * (3 + len(before)),
        out_specs=(spec(VMEM),) * 2,
        compiler_params=params(),
        cost_estimate=pl.CostEstimate(flops=partial.size * 2, bytes_accessed=partial.size * 2, transcendentals=0),
    )(v, partial, square, *before)


def finish_kernel(count_u, count_v, all_ref, v_ref, w0_ref, w1_ref, res0_ref, res1_ref, u_ref, next_ref, scale_ref):
    nv = v_ref.shape[-1]
    everyone = jnp.sum(all_ref[...], axis=0)
    ww, wv, vv, uu = [everyone[:, n : n + 1] for n in range(4)]
    beta = jnp.sqrt(uu / count_u + epsilon)
    inverse = 1.0 / beta
    square = ww * inverse * inverse - 2.0 * wv + vv * beta * beta
    alpha = jnp.sqrt(jnp.maximum(square, 0.0) / count_v + epsilon)
    spread = [jnp.broadcast_to(x, (1, nv)) for x in (beta, inverse, 1.0 / alpha)]
    b, ib, ia = spread
    for f, (res_ref, w_ref) in enumerate(((res0_ref, w0_ref), (res1_ref, w1_ref))):
        u_ref[f] = res_ref[...] * ib
        next_ref[f] = (w_ref[...] * ib - v_ref[f] * b) * ia
    scale_ref[0] = beta[0, 0]
    scale_ref[1] = alpha[0, 0]


def finish(everyone, v, w0, w1, res0, res1, devices):
    count_u = float(2 * res0.size * devices)
    count_v = float(v.size * devices)
    return pl.pallas_call(
        functools.partial(finish_kernel, count_u, count_v),
        out_shape=(
            jax.ShapeDtypeStruct((2, *res0.shape), F32),
            jax.ShapeDtypeStruct(v.shape, F32),
            jax.ShapeDtypeStruct((2,), F32),
        ),
        in_specs=[spec(VMEM)] * 6,
        out_specs=(spec(VMEM), spec(VMEM), spec(SMEM)),
        compiler_params=params(),
        cost_estimate=pl.CostEstimate(flops=v.size * 16, bytes_accessed=v.size * 16, transcendentals=0),
        name="finish",
    )(everyone, v, w0, w1, res0, res1)


def body(left, right, ranks, v, u_prev, alpha_prev):
    frequencies, rows, cols = ranks.shape
    tile = left.shape[2] // rows
    rank_full = left.shape[3] // cols
    nv = v.shape[3]
    peers = lax.axis_size(TROW)
    chips = lax.axis_size("tcol_0")
    devices = peers * lax.axis_size(TCOL)
    dims = (tile, rank_full, rows, cols, nv, v.shape[2], peers)
    core = jnp.stack([lax.axis_index("tcol_0"), lax.axis_index("tcol_1")]).astype(jnp.int32)

    def exchange(value, axes):
        return lax.all_to_all(value, axes, split_axis=0, concat_axis=0, tiled=True)

    def swapped(value):
        return lax.ppermute(value, "tcol_1", [(0, 1), (1, 0)])

    def along_z(value, step):
        return lax.ppermute(value, "tcol_0", [(i, (i + step) % chips) for i in range(chips)])

    sources = prepare(v, peers)
    gathered = []
    for f in range(frequencies):
        gathered.append(exchange(sources[f], TROW))
    results = []
    for f in range(frequencies):
        send, kept, kept_left = project(f, core, ranks, gathered[f], right, left, dims)
        other = swapped(send)
        own, *pieces = expand(kept, other, kept_left, dims)
        arrived = []
        for d, piece in enumerate(pieces):
            arrived.append(along_z(piece, d + 1))
        res, target, square = residual(f, alpha_prev, u_prev, own, arrived)
        near = [target]
        for d in range(1, chips):
            near.append(along_z(target, chips - d))
        far = []
        for d in range(chips):
            far.append(swapped(near[d]))
        back, far_right, far_left = near_back(f, core, ranks, near, right, left, dims)
        partial = adjoint(f, core, ranks, back, far_right, far_left, far, dims)
        results.append((res, square, exchange(partial, TROW)))
    (res0, square0, first), (res1, square1, second) = results
    w0, stats0 = sums(0, v, first, square0, ())
    w1, stats = sums(1, v, second, square1, (stats0,))
    everyone = exchange(jnp.broadcast_to(stats, (devices, *stats.shape)), TROW_TCOL)
    return finish(everyone, v, w0, w1, res0, res1, devices)


def solution(mesh):
    finer = Mesh(mesh.devices.reshape(4, 4, 4, 2), ("trow_0", "trow_1", "tcol_0", "tcol_1"))
    placed = (
        P(None, None, TROW, TCOL),
        P(None, None, TCOL, TROW),
        P(None, TROW, TCOL),
        P(None, None, TCOL_TROW, None),
        P(None, None, TROW_TCOL, None),
        P(),
    )
    return jax.shard_map(
        body,
        mesh=finer,
        in_specs=placed,
        out_specs=(P(None, None, TROW_TCOL, None), P(None, None, TCOL_TROW, None), P()),
        check_vma=False,
    )
```

```python
import functools

import jax
import jax.numpy as jnp
from jax import lax
from jax.experimental import pallas as pl
from jax.experimental.pallas import tpu as pltpu
from jax.sharding import Mesh
from jax.sharding import PartitionSpec as P


TROW = ("trow_0", "trow_1")
TCOL = ("tcol_0", "tcol_1")
TROW_TCOL = ("trow_0", "trow_1", "tcol_0", "tcol_1")
TCOL_TROW = ("tcol_0", "tcol_1", "trow_0", "trow_1")

epsilon = 1e-06
BF = jnp.bfloat16
F32 = jnp.float32
VMEM = pltpu.MemorySpace.VMEM
SMEM = pltpu.MemorySpace.SMEM
HBM = pltpu.MemorySpace.HBM


def spec(space):
    return pl.BlockSpec(memory_space=space)


def in_hbm(value):
    return pltpu.with_memory_space_constraint(value, HBM)


def params(mib=16):
    return pltpu.CompilerParams(vmem_limit_bytes=mib * 1024 * 1024)


def rank_lanes(ranks_of, count, width, rank_full):
    lane = lax.broadcasted_iota(jnp.int32, (8, width), 1)
    limit = jnp.full((8, width), ranks_of(0), jnp.int32)
    for tile in range(1, count):
        limit = jnp.where(lane >= tile * rank_full, ranks_of(tile) + tile * rank_full, limit)
    return (lane < limit)[:1]


def conjugated(stacked, real, imag, half):
    a = jnp.dot(stacked, real, preferred_element_type=F32)
    b = jnp.dot(stacked, imag, preferred_element_type=F32)
    return a[:half] + b[half:], a[half:] - b[:half]


def regroup(first, second, rank_full):
    even = jnp.concatenate([first[:, :rank_full], second[:, :rank_full]], axis=1)
    odd = jnp.concatenate([first[:, rank_full:], second[:, rank_full:]], axis=1)
    return even, odd


def turned(block, half):
    return jnp.concatenate([-block[half:], block[:half]], axis=0)


def prepare_kernel(v_ref, *out_refs):
    for f, ref in enumerate(out_refs):
        ref[...] = v_ref[f].astype(BF)


def prepare(v):
    frequencies = v.shape[0]
    return pl.pallas_call(
        prepare_kernel,
        out_shape=(jax.ShapeDtypeStruct(v.shape[1:], BF),) * frequencies,
        in_specs=[spec(VMEM)],
        out_specs=(spec(VMEM),) * frequencies,
        compiler_params=params(4),
        cost_estimate=pl.CostEstimate(flops=v.size, bytes_accessed=v.size * 6, transcendentals=0),
        name="prepare",
    )(v)


def pack_kernel(axis, *refs):
    parts, out_ref = refs[:-1], refs[-1]
    me = lax.axis_index(axis)
    for d, ref in enumerate(parts):
        out_ref[lax.rem(me + d, len(parts))] = ref[...]


def pack(axis, parts):
    return pl.pallas_call(
        functools.partial(pack_kernel, axis),
        out_shape=jax.ShapeDtypeStruct((len(parts), *parts[0].shape), BF),
        in_specs=[spec(VMEM)] * len(parts),
        out_specs=spec(VMEM),
        compiler_params=params(4),
        cost_estimate=pl.CostEstimate(flops=parts[0].size, bytes_accessed=parts[0].size * 16, transcendentals=0),
    )(*parts)


def load_kernel(*refs):
    factor_ref, outs, sem = refs[-4], refs[-3:-1], refs[-1]
    wait_all(run_all([pltpu.make_async_copy(factor_ref.at[f], out, sem.at[f]) for f, out in enumerate(outs)]))


def load(factor, after=()):
    shape = jax.ShapeDtypeStruct(factor.shape[1:], BF)
    return pl.pallas_call(
        load_kernel,
        out_shape=(shape,) * 2,
        in_specs=[spec(SMEM)] * len(after) + [spec(HBM)],
        out_specs=(spec(VMEM),) * 2,
        scratch_shapes=[pltpu.SemaphoreType.DMA((2,))],
        compiler_params=params(2),
        cost_estimate=pl.CostEstimate(flops=1000000, bytes_accessed=factor.size * 4, transcendentals=0),
    )(*after, in_hbm(factor))


def run_all(copies):
    for copy in copies:
        copy.start()
    return copies


def wait_all(copies):
    for copy in copies:
        copy.wait()


def sides(half):
    z, c = lax.axis_index("tcol_0"), lax.axis_index("tcol_1")
    chips = [2 * lax.rem(z + d, half) for d in range(half)]
    return [chip + c for chip in chips], [chip + (1 - c) for chip in chips]


def tile_of(factor_ref, index, tile):
    at = pl.ds(pl.multiple_of(index * tile, tile), tile)
    return factor_ref[0, at, :], factor_ref[1, at, :]


def expanded(factor, grouped):
    both = jnp.concatenate(factor, axis=1)
    return lax.dot_general(both, grouped, (((1,), (1,)), ((), ())), preferred_element_type=F32)


def masked(kept, real, imag):
    return jnp.where(kept, real, 0.0).astype(BF), jnp.where(kept, imag, 0.0).astype(BF)


def regroup_all(blocks, grouped, outer, inner, rank_full, nv):
    wide = outer * rank_full
    pair = 2 * rank_full
    for o in range(0, outer, 2):
        for i in range(0, inner, 2):
            lanes = slice(i * rank_full, i * rank_full + pair)
            even, odd = regroup(blocks[o, :, lanes], blocks[o + 1, :, lanes], rank_full)
            at = o * rank_full
            for n, block in enumerate((even, odd)):
                grouped[i + n, :, at : at + pair] = block
                grouped[i + n, :, wide + at : wide + at + pair] = turned(block, nv)


def project_kernel(f, dims, axes, ranks_ref, packed_ref, *refs):
    tile, rank_full, rows, cols, nv, share, _ = dims
    arrived, (right_ref, left_ref, send_ref, kept_ref, stored, proj, grouped) = refs[:-7], refs[-7:]
    near, far = sides(rows // 2)
    side = 1 + len(arrived)
    me = lax.axis_index(axes[1])
    for e, ref in enumerate((packed_ref, *arrived)):
        other = lax.rem(me + e, side)
        for n in range(side):
            r = n * side + other if axes[1] == TROW[1] else other * side + n
            at = pl.ds(pl.multiple_of(r * share, share), share)
            for part in range(2):
                stored[part, at, :] = ref[n, part]
    for j in range(cols):
        at = slice(j * tile, (j + 1) * tile)
        stacked = jnp.concatenate([stored[0, at].T, stored[1, at].T], axis=0)
        real, imag = conjugated(stacked, right_ref[0, at, :], right_ref[1, at, :], nv)
        kept = rank_lanes(lambda i: ranks_ref[j, f, i], rows, rows * rank_full, rank_full)
        proj[j, :nv], proj[j, nv:] = masked(kept, real, imag)
    regroup_all(proj, grouped, cols, rows, rank_full, nv)
    for d in range(rows // 2):
        out = expanded(tile_of(left_ref, far[d], tile), grouped[far[d]])
        send_ref[d, 0] = out[:, :nv]
        send_ref[d, 1] = out[:, nv:]
        kept_ref[d] = grouped[near[d]]


def project(f, ranks, axes, packed, arrived, right, left, dims):
    tile, rank_full, rows, cols, nv, _, _ = dims
    half = rows // 2
    return pl.pallas_call(
        functools.partial(project_kernel, f, dims, axes),
        out_shape=(
            jax.ShapeDtypeStruct((half, 2, tile, nv), F32),
            jax.ShapeDtypeStruct((half, 2 * nv, 2 * cols * rank_full), BF),
        ),
        in_specs=[spec(SMEM)] + [spec(VMEM)] * (3 + len(arrived)),
        out_specs=(spec(VMEM),) * 2,
        scratch_shapes=[
            pltpu.VMEM((2, cols * tile, nv), BF),
            pltpu.VMEM((cols, 2 * nv, rows * rank_full), BF),
            pltpu.VMEM((rows, 2 * nv, 2 * cols * rank_full), BF),
        ],
        compiler_params=params(14),
        cost_estimate=pl.CostEstimate(
            flops=12 * rows * cols * tile * rank_full * nv, bytes_accessed=8_000_000, transcendentals=0
        ),
    )(ranks, packed, *arrived, right, left)


def expand_kernel(dims, kept_ref, other_ref, left_ref, own_ref, *piece_refs):
    tile, nv, half = dims[0], dims[4], dims[2] // 2
    near, _ = sides(half)
    for d in list(range(1, half)) + [0]:
        out = expanded(tile_of(left_ref, near[d], tile), kept_ref[d])
        for part in range(2):
            total = out[:, part * nv : (part + 1) * nv] + other_ref[d, part]
            if d == 0:
                own_ref[part] = total
            else:
                piece_refs[d - 1][part] = total.astype(BF)


def expand(kept, other, left, dims):
    tile, rank_full, rows, cols, nv, _, _ = dims
    half = rows // 2
    piece = (2, tile, nv)
    return pl.pallas_call(
        functools.partial(expand_kernel, dims),
        out_shape=(jax.ShapeDtypeStruct(piece, F32),)
        + (jax.ShapeDtypeStruct(piece, BF),) * (half - 1),
        in_specs=[spec(VMEM)] * 3,
        out_specs=(spec(VMEM),) * half,
        compiler_params=params(),
        cost_estimate=pl.CostEstimate(
            flops=4 * rows * cols * tile * rank_full * nv, bytes_accessed=4_000_000, transcendentals=0
        ),
    )(kept, other, left)


def back_of(f, index, target, left_ref, ranks_ref, dims):
    tile, rank_full, _, cols, nv, _, _ = dims
    real, imag = conjugated(target, *tile_of(left_ref, index, tile), nv)
    kept = rank_lanes(lambda j: ranks_ref[j, f, index], cols, cols * rank_full, rank_full)
    whole = [jnp.where(kept, value, 0.0) for value in (real, imag)]
    lead = [value.astype(BF) for value in whole]
    rest = [(value - top.astype(F32)).astype(BF) for value, top in zip(whole, lead)]
    return lead, rest


def near_kernel(f, dims, ranks_ref, left_ref, *refs):
    nv, half = dims[4], dims[2] // 2
    targets, back_ref = refs[:-1], refs[-1]
    near, _ = sides(half)
    for d in range(half):
        for term, parts in enumerate(back_of(f, near[d], targets[d][...], left_ref, ranks_ref, dims)):
            back_ref[term, d, :nv], back_ref[term, d, nv:] = parts


def near_back(f, ranks, targets, left, dims):
    tile, rank_full, rows, cols, nv, _, _ = dims
    half = rows // 2
    return pl.pallas_call(
        functools.partial(near_kernel, f, dims),
        out_shape=jax.ShapeDtypeStruct((2, half, 2 * nv, cols * rank_full), BF),
        in_specs=[spec(SMEM), spec(VMEM)] + [spec(VMEM)] * half,
        out_specs=spec(VMEM),
        compiler_params=params(8),
        cost_estimate=pl.CostEstimate(
            flops=4 * rows * cols * tile * rank_full * nv, bytes_accessed=4_000_000, transcendentals=0
        ),
    )(ranks, left, *targets)


def place(axes, along_first, along_second, side):
    if axes[0] == TROW[0]:
        return along_first * side + along_second
    return along_second * side + along_first


def adjoint_kernel(f, dims, axes, side, ranks_ref, near_ref, right_ref, left_ref, *refs):
    tile, rank_full, rows, cols, nv, share, _ = dims
    half = rows // 2
    targets, piece_refs, (back, grouped, out_ref) = refs[:half], refs[half:-3], refs[-3:]
    near, far = sides(half)
    for d in range(half):
        for term, parts in enumerate(back_of(f, far[d], targets[d][...], left_ref, ranks_ref, dims)):
            back[term, near[d]] = near_ref[term, d]
            back[term, far[d], :nv], back[term, far[d], nv:] = parts
    for term in range(2):
        regroup_all(back.at[term], grouped.at[term], rows, cols, rank_full, nv)
    for j in range(cols):
        factor = tile_of(right_ref, j, tile)
        out = (expanded(factor, grouped[0, j]) + expanded(factor, grouped[1, j])).astype(BF)
        row = 0
        while row < tile:
            r, start = divmod(j * tile + row, share)
            count = min(share - start, tile - row)
            for part in range(2):
                piece = out[row : row + count, part * nv : (part + 1) * nv]
                out_ref[r, part, start : start + count] = piece
            row += count
    me = lax.axis_index(axes[0])
    for d, ref in enumerate(piece_refs):
        for n in range(side):
            ref[n] = out_ref[place(axes, lax.rem(me + d, side), n, side)]


def adjoint(f, ranks, axes, near, right, left, targets, dims):
    tile, rank_full, rows, cols, nv, share, peers = dims
    side = lax.axis_size(axes[0])
    return pl.pallas_call(
        functools.partial(adjoint_kernel, f, dims, axes, side),
        out_shape=(jax.ShapeDtypeStruct((peers // side, 2, share, nv), BF),) * side,
        in_specs=[spec(SMEM)] + [spec(VMEM)] * (3 + len(targets)),
        out_specs=(spec(VMEM),) * side,
        scratch_shapes=[
            pltpu.VMEM((2, rows, 2 * nv, cols * rank_full), BF),
            pltpu.VMEM((2, cols, 2 * nv, 2 * rows * rank_full), BF),
            pltpu.VMEM((peers, 2, share, nv), BF),
        ],
        compiler_params=params(18),
        cost_estimate=pl.CostEstimate(
            flops=12 * rows * cols * tile * rank_full * nv, bytes_accessed=8_000_000, transcendentals=0
        ),
    )(ranks, near, right, left, *targets)


def merge_kernel(axis, *refs):
    half = len(refs) // 2
    parts, own_ref, piece_refs = refs[:half], refs[half], refs[half + 1 :]
    me = lax.axis_index(axis)
    for e in range(half):
        n = lax.rem(me + e, half)
        total = parts[0][n].astype(F32)
        for ref in parts[1:]:
            total = total + ref[n].astype(F32)
        if e == 0:
            own_ref[...] = total
        else:
            piece_refs[e - 1][...] = total


def merge(axis, parts):
    piece = parts[0].shape[1:]
    count = len(parts)
    return pl.pallas_call(
        functools.partial(merge_kernel, axis),
        out_shape=(jax.ShapeDtypeStruct(piece, F32),) * count,
        in_specs=[spec(VMEM)] * count,
        out_specs=(spec(VMEM),) * count,
        compiler_params=params(8),
        cost_estimate=pl.CostEstimate(flops=parts[0].size * 8, bytes_accessed=parts[0].size * 12, transcendentals=0),
    )(*parts)


def folded(value):
    return jnp.sum(value.reshape(-1, 8, value.shape[-1]), axis=0)


def residual_kernel(f, alpha_ref, u_prev_ref, own_ref, *refs):
    pieces, (res_ref, target_ref, square_ref) = refs[:-3], refs[-3:]
    total = own_ref[...] - alpha_ref[0] * u_prev_ref[f]
    for ref in pieces:
        total = total + ref[...].astype(F32)
    res_ref[...] = total
    nv = total.shape[-1]
    for part in range(2):
        target_ref[part * nv : (part + 1) * nv] = total[part].T.astype(BF)
    square_ref[...] = folded(total * total)


def residual(f, alpha_prev, u_prev, own, pieces):
    _, tile, nv = own.shape
    return pl.pallas_call(
        functools.partial(residual_kernel, f),
        out_shape=(
            jax.ShapeDtypeStruct(own.shape, F32),
            jax.ShapeDtypeStruct((2 * nv, tile), BF),
            jax.ShapeDtypeStruct((8, nv), F32),
        ),
        in_specs=[spec(SMEM)] + [spec(VMEM)] * (2 + len(pieces)),
        out_specs=(spec(VMEM),) * 3,
        compiler_params=params(),
        cost_estimate=pl.CostEstimate(flops=own.size * 8, bytes_accessed=own.size * 16, transcendentals=0),
    )(alpha_prev, u_prev, own, *pieces)


def nothing_kernel(out_ref):
    out_ref[...] = jnp.zeros_like(out_ref)


def nothing(nv):
    return pl.pallas_call(
        nothing_kernel,
        out_shape=jax.ShapeDtypeStruct((1, nv), F32),
        out_specs=spec(VMEM),
        compiler_params=params(1),
        cost_estimate=pl.CostEstimate(flops=nv, bytes_accessed=nv * 4, transcendentals=0),
        name="nothing",
    )()


def lane_sums(stats):
    nv = stats[0].shape[-1]
    lane = lax.broadcasted_iota(jnp.int32, (1, nv), 1)
    row = jnp.zeros((1, nv), F32)
    for n, value in enumerate(stats):
        total = jnp.sum(jnp.sum(value, axis=0, keepdims=True), axis=1, keepdims=True)
        row = jnp.where(lane == n, total, row)
    return row


def sums_kernel(f, v_ref, square_ref, own_ref, *refs):
    arrived, (before_ref, w_ref, stats_ref) = refs[:-3], refs[-3:]
    total = own_ref[...]
    for ref in arrived:
        total = total + ref[...]
    w_ref[...] = total
    v = v_ref[f]
    row = lane_sums([folded(total * total), folded(total * v), folded(v * v), square_ref[...]])
    stats_ref[...] = row + before_ref[...]


def sums(f, v, square, own, arrived, before):
    nv = v.shape[-1]
    return pl.pallas_call(
        functools.partial(sums_kernel, f),
        out_shape=(jax.ShapeDtypeStruct(v.shape[1:], F32), jax.ShapeDtypeStruct((1, nv), F32)),
        in_specs=[spec(VMEM)] * (4 + len(arrived)),
        out_specs=(spec(VMEM),) * 2,
        compiler_params=params(8),
        cost_estimate=pl.CostEstimate(flops=own.size * 8, bytes_accessed=own.size * 12, transcendentals=0),
    )(v, square, own, *arrived, before)


def finish_kernel(count_u, count_v, all_ref, v_ref, w0_ref, w1_ref, res0_ref, res1_ref, u_ref, next_ref, scale_ref):
    nv = v_ref.shape[-1]
    everyone = jnp.sum(all_ref[...], axis=0)
    ww, wv, vv, uu = [everyone[:, n : n + 1] for n in range(4)]
    beta = jnp.sqrt(uu / count_u + epsilon)
    inverse = 1.0 / beta
    square = ww * inverse * inverse - 2.0 * wv + vv * beta * beta
    alpha = jnp.sqrt(jnp.maximum(square, 0.0) / count_v + epsilon)
    spread = [jnp.broadcast_to(x, (1, nv)) for x in (beta, inverse, 1.0 / alpha)]
    b, ib, ia = spread
    u_ref[0] = res0_ref[...] * ib
    u_ref[1] = res1_ref[...] * ib
    for f, w_ref in enumerate((w0_ref, w1_ref)):
        next_ref[f] = (w_ref[...] * ib - v_ref[f] * b) * ia
    scale_ref[0] = beta[0, 0]
    scale_ref[1] = alpha[0, 0]


def finish(everyone, v, w0, w1, res0, res1, devices):
    count_u = float(2 * res0.size * devices)
    count_v = float(v.size * devices)
    return pl.pallas_call(
        functools.partial(finish_kernel, count_u, count_v),
        out_shape=(
            jax.ShapeDtypeStruct((2, *res0.shape), F32),
            jax.ShapeDtypeStruct(v.shape, F32),
            jax.ShapeDtypeStruct((2,), F32),
        ),
        in_specs=[spec(VMEM)] * 6,
        out_specs=(spec(VMEM), spec(VMEM), spec(SMEM)),
        compiler_params=params(),
        cost_estimate=pl.CostEstimate(flops=v.size * 16, bytes_accessed=v.size * 16, transcendentals=0),
        name="finish",
    )(everyone, v, w0, w1, res0, res1)


def body(left, right, ranks, v, u_prev, alpha_prev):
    frequencies, rows, cols = ranks.shape
    tile = left.shape[2] // rows
    rank_full = left.shape[3] // cols
    nv = v.shape[3]
    ranks = jnp.transpose(ranks, (2, 0, 1))
    peers = lax.axis_size(TROW)
    chips = lax.axis_size("tcol_0")
    devices = peers * lax.axis_size(TCOL)
    dims = (tile, rank_full, rows, cols, nv, v.shape[2], peers)

    def exchange(value, axes):
        return lax.all_to_all(value, axes, split_axis=0, concat_axis=0, tiled=True)

    def swapped(value):
        return lax.ppermute(value, "tcol_1", [(0, 1), (1, 0)])

    def along(value, axis, step):
        size = lax.axis_size(axis)
        return lax.ppermute(value, axis, [(i, (i + step) % size) for i in range(size)])

    def from_others(value, axis):
        size = lax.axis_size(axis)
        arrived = []
        for d in range(1, size):
            arrived.append(along(value, axis, size - d))
        return arrived

    sources = prepare(v)
    ways = [(TROW[1], TROW[0]), (TROW[0], TROW[1])]
    stage = [[sources[f], *from_others(sources[f], ways[f][0])] for f in range(frequencies)]
    rights = load(right, (ranks, alpha_prev))
    lefts = load(left)
    packed = [pack(ways[f][0], stage[f]) for f in range(frequencies)]
    arrivals = [from_others(packed[f], ways[f][1]) for f in range(frequencies)]
    squares, residuals, merged = [], [], []
    for f in range(frequencies):
        send, kept = project(f, ranks, ways[f], packed[f], arrivals[f], rights[f], lefts[f], dims)
        other = swapped(send)
        own, *pieces = expand(kept, other, lefts[f], dims)
        arrived = []
        for d, piece in enumerate(pieces):
            arrived.append(along(piece, "tcol_0", d + 1))
        res, target, square = residual(f, alpha_prev, u_prev, own, arrived)
        near = [target, *from_others(target, "tcol_0")]
        far = []
        for d in range(chips):
            far.append(swapped(near[d]))
        back = near_back(f, ranks, near, lefts[f], dims)
        way = ways[0]
        mine, *others = adjoint(f, ranks, way, back, rights[f], lefts[f], far, dims)
        parts = [mine]
        for d, piece in enumerate(others):
            parts.append(along(piece, way[0], d + 1))
        mine, *others = merge(way[1], parts)
        parts = []
        for d, piece in enumerate(others):
            parts.append(along(piece, way[1], d + 1))
        merged.append((mine, parts))
        residuals.append(res)
        squares.append(square)
    ws, stats = [], nothing(nv)
    for f in range(frequencies):
        w, stats = sums(f, v, squares[f], *merged[f], stats)
        ws.append(w)
    everyone = exchange(jnp.broadcast_to(stats, (devices, *stats.shape)), TROW_TCOL)
    return finish(everyone, v, *ws, *residuals, devices)


def solution(mesh):
    finer = Mesh(mesh.devices.reshape(4, 4, 4, 2), ("trow_0", "trow_1", "tcol_0", "tcol_1"))
    placed = (
        P(None, None, TROW, TCOL),
        P(None, None, TCOL, TROW),
        P(None, TROW, TCOL),
        P(None, None, TCOL_TROW, None),
        P(None, None, TROW_TCOL, None),
        P(),
    )
    return jax.shard_map(
        body,
        mesh=finer,
        in_specs=placed,
        out_specs=(P(None, None, TROW_TCOL, None), P(None, None, TCOL_TROW, None), P()),
        check_vma=False,
    )
```
